32 devices in a mesh: groups: 2 (over y), blk: 4 (over z), tile: 2 (over x), sub: 2 (over core).
Axes of the slice: x: 2, y: 2, z: 4, core: 2. Of those that a mesh axis runs over, the one named last changes fastest.
Arguments:
- raw_desc: bfloat16 [4096, 1536], P(('groups', 'blk', 'tile')), parts along dimension 0, may hold values from -11 to 11
- desc_mean: float32 [1536], replicated, may hold values from -6 to 6
- whitening: bfloat16 [1536, 256], P(None, 'sub'), may hold values from -0.15625 to 0.15625
Outputs:
- augmented: float32 [4096, 256], P(('groups', 'blk', 'tile'), 'sub'), parts along dimension 0
The draws below stay inside these ranges and needn't reach their ends.
There are 2 independent parts, one for each index of `groups`. The reference program is written for one: setup_inputs(seed, part) draws one part's arguments, and reference() takes and returns one part's arrays. A program takes and returns all parts, laid end to end along the dimension named above; an argument that names none is the same for every part. Nothing has to cross between parts.
All inputs are finite; a program needn't handle non-finite values.
Results may differ from the reference program's by a relative error of at most 0.0055.
The reference program's roundings to bfloat16 on the way count: a program that leaves them out, or rounds other values in their place, can miss the bound.
Values may be sent and summed in bfloat16 or wider, within the bound.
A program may use at most 128 MiB of HBM per device.

```python
import math
import jax
import jax.numpy as jnp
from jax import lax

RAW = 1536
WHITE = 256
IMAGES = 2048


def draw_raw_desc(key, part):
    first = jax.random.fold_in(jax.random.fold_in(key, 11), 0)
    values = jnp.clip(jax.random.normal(first, (IMAGES, RAW), jnp.float32), -6.0, 6.0)
    return values.astype(jnp.bfloat16)


def block_scale(key, shape, shards, low, high):
    level, own = 1.0, jax.random.fold_in(key, 6)
    for axis_at, parts in shards:
        heights = jnp.exp(jax.random.uniform(jax.random.fold_in(own, axis_at), (parts,), jnp.float32, low / len(shards), high / len(shards)))
        level = level * jnp.repeat(heights, shape[axis_at] // parts).reshape([-1 if axis == axis_at else 1 for axis in range(len(shape))])
    return level


def noise(key, shape, spread, reach, cuts=(), held_as=jnp.bfloat16):
    drawn = jax.random.normal(key, shape, jnp.float32) * spread
    if len(cuts) > 0:
        drawn = block_scale(key, shape, cuts, -0.22, 0.18) * drawn
    return jnp.clip(drawn, min=-reach, max=reach).astype(held_as)


def setup_inputs(seed: int = 0, part: int = 0) -> dict:
    key_list = jax.random.split(jax.random.key(seed), 4)
    part_splits = jax.random.split(jax.random.fold_in(key_list[3], part), 4)
    raw_desc = draw_raw_desc(jax.random.fold_in(jax.random.fold_in(key_list[3], part), 71), part)
    desc_mean = noise(key_list[1], (RAW,), 1.0, 6.0, (), jnp.float32)
    whitening = noise(key_list[2], (RAW, WHITE), RAW ** -0.5, 0.15625, ((1, 2),))
    return dict(raw_desc=raw_desc, desc_mean=desc_mean, whitening=whitening)


beta = 0.125

def reference(raw_desc, desc_mean, whitening):
    centred = (raw_desc.astype(jnp.float32) - desc_mean).astype(jnp.bfloat16)
    feats = jnp.dot(centred, whitening, preferred_element_type=jnp.float32).astype(jnp.bfloat16)
    feats_full = feats.astype(jnp.float32)
    images = feats.shape[0]
    block = math.gcd(images, 512)
    key_index = jnp.arange(images, dtype=jnp.int32)

    def one_block(which):
        start = (which * block).astype(jnp.int32)
        queries = lax.dynamic_slice_in_dim(feats_full, start, block, 0)
        scores = beta * jnp.dot(queries, feats_full.T, precision=lax.Precision.HIGHEST, preferred_element_type=jnp.float32)
        query_index = start + jnp.arange(block, dtype=jnp.int32)
        masked = query_index[:, None] == key_index[None, :]
        scores = jnp.where(masked, -jnp.inf, scores)
        top = lax.optimization_barrier(jnp.max(scores, axis=1))
        expo = jnp.where(masked, 0.0, jnp.exp(scores - top[:, None]))
        total = lax.optimization_barrier(jnp.sum(expo, axis=1))
        summed = jnp.dot(expo.astype(jnp.bfloat16), feats, preferred_element_type=jnp.float32)
        return summed / total[:, None]
    gathered = lax.map(one_block, jnp.arange(images // block, dtype=jnp.int32))
    gathered = gathered.reshape(images, feats.shape[1])
    mixed = feats_full + gathered
    return mixed * lax.rsqrt(lax.optimization_barrier(jnp.sum(mixed * mixed, axis=1, keepdims=True)) + 1e-06)
```

```python
import functools

import jax
import jax.numpy as jnp
from jax import lax
from jax.experimental import pallas as pl
from jax.experimental.pallas import tpu as pltpu
from jax.sharding import PartitionSpec as P

beta = 0.125
lowest = -1e30
MESH = pl.DeviceIdType.MESH


def repeat(count, body):
    if count <= 8:
        for k in range(count):
            body(k)
    else:
        lax.fori_loop(0, count, lambda k, _: (body(k), 0)[1], 0)


def peer_of(me, k, count):
    if count == 4:
        if k == 0:
            return me + 1 - 2 * lax.rem(me, 2)
        if k == 1:
            return lax.rem(me + 2, 4)
        return 3 - me
    return lax.rem(me + k + 1, count)


def kernel(
    blks, tiles, chunks,
    raw_hbm, mean_ref, white_hbm, out_ref,
    raw, white, feats, keys, acc, stat, put_acc, put_stat, got_acc, got_stat,
    raw_sem, white_sem, pair_send, pair_recv, own_send, fwd_send, key_recv,
    part_send, part_recv,
):
    z, x, s = lax.axis_index("blk"), lax.axis_index("tile"), lax.axis_index("sub")
    other = 1 - s
    rows, width = feats.shape[1], feats.shape[2]
    part = rows // 2
    step = rows // chunks
    load_white = pltpu.make_async_copy(white_hbm, white, white_sem)
    load_white.start()
    loads = []
    for c in range(chunks):
        at = pl.ds(c * step, step)
        loads.append(pltpu.make_async_copy(raw_hbm.at[at], raw.at[at], raw_sem.at[c]))
        loads[-1].start()

    barrier = pltpu.get_barrier_semaphore()
    pl.semaphore_signal(barrier, inc=1, device_id={"sub": other}, device_id_type=MESH)

    def greet_z(k):
        for r in range(2):
            pl.semaphore_signal(
                barrier, inc=1, device_id={"blk": peer_of(z, k, blks), "sub": r},
                device_id_type=MESH,
            )

    def greet_x(k):
        for r in range(2):
            pl.semaphore_signal(
                barrier, inc=1, device_id={"tile": peer_of(x, k, tiles), "sub": r},
                device_id_type=MESH,
            )

    repeat(blks - 1, greet_z)
    repeat(tiles - 1, greet_x)

    def piece(r):
        return feats.at[s, pl.ds(r * part, part)]

    def slot(zz, xx):
        return zz * tiles + xx

    def own_to_z(k, r):
        return pltpu.make_async_remote_copy(
            piece(r), keys.at[slot(z, x), s], own_send.at[k, r], key_recv.at[slot(z, x), s],
            device_id={"blk": peer_of(z, k, blks), "sub": r}, device_id_type=MESH,
        )

    def own_to_x(k, r):
        return pltpu.make_async_remote_copy(
            piece(r), keys.at[slot(z, x), s], own_send.at[blks - 1 + k, r],
            key_recv.at[slot(z, x), s],
            device_id={"tile": peer_of(x, k, tiles), "sub": r}, device_id_type=MESH,
        )

    def forward(k, j, h):
        block = slot(peer_of(z, k, blks), x)
        return pltpu.make_async_remote_copy(
            keys.at[block, h], keys.at[block, h], fwd_send.at[k, j, h],
            key_recv.at[block, h],
            device_id={"tile": peer_of(x, j, tiles)}, device_id_type=MESH,
        )

    def pair(r):
        return pltpu.make_async_remote_copy(
            piece(r), piece(r), pair_send.at[r], pair_recv.at[r],
            device_id={"sub": other}, device_id_type=MESH,
        )

    mean = mean_ref[...].reshape(1, -1)
    load_white.wait()
    for c in range(chunks):
        loads[c].wait()
        at = pl.ds(c * step, step)
        centred = (raw[at, :].astype(jnp.float32) - mean).astype(jnp.bfloat16)
        half = jnp.dot(centred, white[...], preferred_element_type=jnp.float32)
        feats[s, at, :] = half.astype(jnp.bfloat16)
        if (c + 1) % (chunks // 2) == 0:
            r = (c + 1) // (chunks // 2) - 1
            if r == 0:
                pl.semaphore_wait(barrier, 1 + 2 * (blks - 1) + 2 * (tiles - 1))
            repeat(blks - 1, lambda k: own_to_z(k, r).start())
            repeat(tiles - 1, lambda k: own_to_x(k, r).start())
            pair(r).start()

    def arrived(block, h):
        pltpu.make_async_copy(
            keys.at[block, h], keys.at[block, h], key_recv.at[block, h]
        ).wait()

    def scores_of(k0, k1):
        nt = (((1,), (1,)), ((), ()))
        q = jnp.concatenate([feats[0], feats[1]], axis=1)
        kk = jnp.concatenate([k0, k1], axis=1)
        return beta * lax.dot_general(q, kk, nt, preferred_element_type=jnp.float32), kk

    def attend(block):
        sc, kk = scores_of(keys[block, 0], keys[block, 1])
        old = stat[0]
        top = jnp.maximum(old, jnp.max(sc, axis=1, keepdims=True))
        scale = jnp.exp(old - top)
        expo = jnp.exp(sc - top[:, :1])
        stat[0] = top
        stat[1] = stat[1] * scale + jnp.sum(expo, axis=1, keepdims=True)
        acc[...] = acc[...] * scale[:, :1] + jnp.dot(
            expo.astype(jnp.bfloat16), kk, preferred_element_type=jnp.float32
        )

    for r in range(2):
        pair(r).wait()
    mine = pl.ds(pl.multiple_of(s * part, part), part)
    sc, kk = scores_of(feats[0, mine, :], feats[1, mine, :])
    query = lax.broadcasted_iota(jnp.int32, sc.shape, 0)
    key = lax.broadcasted_iota(jnp.int32, sc.shape, 1) + s * part
    masked = query == key
    sc = jnp.where(masked, lowest, sc)
    top = jnp.max(sc, axis=1, keepdims=True)
    expo = jnp.where(masked, 0.0, jnp.exp(sc - top))
    stat[0] = jnp.broadcast_to(top, stat.shape[1:])
    stat[1] = jnp.broadcast_to(jnp.sum(expo, axis=1, keepdims=True), stat.shape[1:])
    acc[...] = jnp.dot(expo.astype(jnp.bfloat16), kk, preferred_element_type=jnp.float32)

    def from_z(k):
        block = slot(peer_of(z, k, blks), x)
        for h in range(2):
            arrived(block, h)
            repeat(tiles - 1, lambda j: forward(k, j, h).start())
        attend(block)

    def from_x(k):
        block = slot(z, peer_of(x, k, tiles))
        for h in range(2):
            arrived(block, h)
        attend(block)

    def diagonal(k):
        def one(j):
            block = slot(peer_of(z, k, blks), peer_of(x, j, tiles))
            for h in range(2):
                arrived(block, h)
            attend(block)
        repeat(tiles - 1, one)

    repeat(tiles - 1, from_x)
    repeat(blks - 1, from_z)
    repeat(blks - 1, diagonal)

    put_acc[...] = acc[...].astype(jnp.bfloat16)
    lane = lax.broadcasted_iota(jnp.int32, put_stat.shape, 1)
    put_stat[...] = jnp.where(lane < width // 2, stat[0], stat[1])
    send_acc = pltpu.make_async_remote_copy(
        put_acc, got_acc, part_send.at[0], part_recv.at[0],
        device_id={"sub": other}, device_id_type=MESH,
    )
    send_stat = pltpu.make_async_remote_copy(
        put_stat, got_stat, part_send.at[1], part_recv.at[1],
        device_id={"sub": other}, device_id_type=MESH,
    )
    send_stat.start()
    send_acc.start()

    def own_sent(k):
        for r in range(2):
            own_to_z(k, r).wait_send()

    def own_sent_x(k):
        for r in range(2):
            own_to_x(k, r).wait_send()

    def fwd_sent(k):
        def one(j):
            for h in range(2):
                forward(k, j, h).wait_send()
        repeat(tiles - 1, one)

    repeat(blks - 1, own_sent)
    repeat(tiles - 1, own_sent_x)
    repeat(blks - 1, fwd_sent)

    send_stat.wait()
    my_top, my_total = stat[0][:, :1], stat[1][:, :1]
    its_top, its_total = got_stat[:, :1], got_stat[:, width // 2:width // 2 + 1]
    top = jnp.maximum(my_top, its_top)
    mine_by, its_by = jnp.exp(my_top - top), jnp.exp(its_top - top)
    total = my_total * mine_by + its_total * its_by
    mine_by, its_by = mine_by / total, its_by / total
    send_acc.wait()
    gathered = acc[...] * mine_by + got_acc[...].astype(jnp.float32) * its_by
    whole = jnp.concatenate([feats[0], feats[1]], axis=1).astype(jnp.float32)
    mixed = whole + gathered
    squares = jnp.sum(mixed * mixed, axis=1, keepdims=True)
    wanted = jnp.where(s == 0, mixed[:, :width], mixed[:, width:])
    out_ref[...] = wanted * lax.rsqrt(squares + 1e-06)


def local(raw_desc, desc_mean, whitening):
    rows, depth = raw_desc.shape
    width = whitening.shape[1]
    blks, tiles = lax.axis_size("blk"), lax.axis_size("tile")
    chunks = 4
    part = rows // 2
    chips = blks * tiles
    vmem = pl.BlockSpec(memory_space=pltpu.VMEM)
    hbm = pl.BlockSpec(memory_space=pl.ANY)
    dma = pltpu.SemaphoreType.DMA
    bf16, f32 = jnp.bfloat16, jnp.float32
    return pl.pallas_call(
        functools.partial(kernel, blks, tiles, chunks),
        out_shape=jax.ShapeDtypeStruct((rows, width), f32),
        in_specs=[hbm, vmem, hbm],
        out_specs=vmem,
        scratch_shapes=[
            pltpu.VMEM((rows, depth), bf16),
            pltpu.VMEM((depth, width), bf16),
            pltpu.VMEM((2, rows, width), bf16),
            pltpu.VMEM((chips, 2, part, width), bf16),
            pltpu.VMEM((rows, 2 * width), f32),
            pltpu.VMEM((2, rows, width), f32),
            pltpu.VMEM((rows, 2 * width), bf16),
            pltpu.VMEM((rows, width), f32),
            pltpu.VMEM((rows, 2 * width), bf16),
            pltpu.VMEM((rows, width), f32),
            dma((chunks,)),
            dma,
            dma((2,)),
            dma((2,)),
            dma((blks - 1 + tiles - 1, 2)),
            dma((blks - 1, tiles - 1, 2)),
            dma((chips, 2)),
            dma((2,)),
            dma((2,)),
        ],
        compiler_params=pltpu.CompilerParams(collective_id=0, has_side_effects=True),
        name="augment",
    )(raw_desc, desc_mean, whitening)


def solution(mesh):
    return jax.shard_map(
        local,
        mesh=mesh,
        in_specs=(P(("groups", "blk", "tile"), None), P(), P(None, "sub")),
        out_specs=P(("groups", "blk", "tile"), "sub"),
        check_vma=False,
    )
```

```python
import functools

import jax
import jax.numpy as jnp
from jax import lax
from jax.experimental import pallas as pl
from jax.experimental.pallas import tpu as pltpu
from jax.sharding import PartitionSpec as P

beta = 0.125
lowest = -1e30
MESH = pl.DeviceIdType.MESH


def repeat(count, body):
    if count <= 8:
        for k in range(count):
            body(k)
    else:
        lax.fori_loop(0, count, lambda k, _: (body(k), 0)[1], 0)


def peer_of(me, k, count):
    if count == 4:
        if k == 0:
            return me + 1 - 2 * lax.rem(me, 2)
        if k == 1:
            return lax.rem(me + 2, 4)
        return 3 - me
    return lax.rem(me + k + 1, count)


def kernel(
    blks, tiles, chunks,
    raw_hbm, mean_ref, white_hbm, out_ref,
    raw, white, feats, keys, acc, stat, put_acc, put_stat, got_acc, got_stat,
    raw_sem, white_sem, pair_send, pair_recv, own_send, fwd_send, key_recv,
    part_send, part_recv,
):
    z, x, s = lax.axis_index("blk"), lax.axis_index("tile"), lax.axis_index("sub")
    other = 1 - s
    rows, width = feats.shape[1], feats.shape[2]
    part = rows // 2
    step = rows // chunks
    load_white = pltpu.make_async_copy(white_hbm, white, white_sem)
    load_white.start()
    loads = []
    for c in range(chunks):
        at = pl.ds(c * step, step)
        loads.append(pltpu.make_async_copy(raw_hbm.at[at], raw.at[at], raw_sem.at[c]))
        loads[-1].start()

    barrier = pltpu.get_barrier_semaphore()
    pl.semaphore_signal(barrier, inc=1, device_id={"sub": other}, device_id_type=MESH)

    def greet_z(k):
        for r in range(2):
            pl.semaphore_signal(
                barrier, inc=1, device_id={"blk": peer_of(z, k, blks), "sub": r},
                device_id_type=MESH,
            )

    def greet_x(k):
        for r in range(2):
            pl.semaphore_signal(
                barrier, inc=1, device_id={"tile": peer_of(x, k, tiles), "sub": r},
                device_id_type=MESH,
            )

    repeat(blks - 1, greet_z)
    repeat(tiles - 1, greet_x)

    def piece(r):
        return feats.at[s, pl.ds(r * part, part)]

    def slot(zz, xx):
        return zz * tiles + xx

    def own_to_z(k, r):
        return pltpu.make_async_remote_copy(
            piece(r), keys.at[slot(z, x), s], own_send.at[k, r], key_recv.at[slot(z, x), s],
            device_id={"blk": peer_of(z, k, blks), "sub": r}, device_id_type=MESH,
        )

    def own_to_x(k, r):
        return pltpu.make_async_remote_copy(
            piece(r), keys.at[slot(z, x), s], own_send.at[blks - 1 + k, r],
            key_recv.at[slot(z, x), s],
            device_id={"tile": peer_of(x, k, tiles), "sub": r}, device_id_type=MESH,
        )

    def forward(k, j, h):
        block = slot(peer_of(z, k, blks), x)
        return pltpu.make_async_remote_copy(
            keys.at[block, h], keys.at[block, h], fwd_send.at[k, j, h],
            key_recv.at[block, h],
            device_id={"tile": peer_of(x, j, tiles)}, device_id_type=MESH,
        )

    def pair(r):
        return pltpu.make_async_remote_copy(
            piece(r), piece(r), pair_send.at[r], pair_recv.at[r],
            device_id={"sub": other}, device_id_type=MESH,
        )

    mean = mean_ref[...].reshape(1, -1)
    load_white.wait()
    for c in range(chunks):
        loads[c].wait()
        at = pl.ds(c * step, step)
        centred = (raw[at, :].astype(jnp.float32) - mean).astype(jnp.bfloat16)
        half = jnp.dot(centred, white[...], preferred_element_type=jnp.float32)
        feats[s, at, :] = half.astype(jnp.bfloat16)
        if (c + 1) % (chunks // 2) == 0:
            r = (c + 1) // (chunks // 2) - 1
            if r == 0:
                pl.semaphore_wait(barrier, 1 + 2 * (blks - 1) + 2 * (tiles - 1))
            repeat(blks - 1, lambda k: own_to_z(k, r).start())
            repeat(tiles - 1, lambda k: own_to_x(k, r).start())
            pair(r).start()

    def arrived(block, h):
        pltpu.make_async_copy(
            keys.at[block, h], keys.at[block, h], key_recv.at[block, h]
        ).wait()

    def scores_of(k0, k1):
        nt = (((1,), (1,)), ((), ()))
        q = jnp.concatenate([feats[0], feats[1]], axis=1)
        kk = jnp.concatenate([k0, k1], axis=1)
        return beta * lax.dot_general(q, kk, nt, preferred_element_type=jnp.float32), kk

    def attend(block):
        sc, kk = scores_of(keys[block, 0], keys[block, 1])
        old = stat[0]
        top = jnp.maximum(old, jnp.max(sc, axis=1, keepdims=True))
        scale = jnp.exp(old - top)
        expo = jnp.exp(sc - top[:, :1])
        stat[0] = top
        stat[1] = stat[1] * scale + jnp.sum(expo, axis=1, keepdims=True)
        acc[...] = acc[...] * scale[:, :1] + jnp.dot(
            expo.astype(jnp.bfloat16), kk, preferred_element_type=jnp.float32
        )

    for r in range(2):
        pair(r).wait()
    mine = pl.ds(pl.multiple_of(s * part, part), part)
    sc, kk = scores_of(feats[0, mine, :], feats[1, mine, :])
    query = lax.broadcasted_iota(jnp.int32, sc.shape, 0)
    key = lax.broadcasted_iota(jnp.int32, sc.shape, 1) + s * part
    masked = query == key
    sc = jnp.where(masked, lowest, sc)
    top = jnp.max(sc, axis=1, keepdims=True)
    expo = jnp.where(masked, 0.0, jnp.exp(sc - top))
    stat[0] = jnp.broadcast_to(top, stat.shape[1:])
    stat[1] = jnp.broadcast_to(jnp.sum(expo, axis=1, keepdims=True), stat.shape[1:])
    acc[...] = jnp.dot(expo.astype(jnp.bfloat16), kk, preferred_element_type=jnp.float32)

    def from_z(k):
        block = slot(peer_of(z, k, blks), x)
        for h in range(2):
            arrived(block, h)
            repeat(tiles - 1, lambda j: forward(k, j, h).start())
        attend(block)

    def from_x(k):
        block = slot(z, peer_of(x, k, tiles))
        for h in range(2):
            arrived(block, h)
        attend(block)

    def diagonal(k):
        def one(j):
            block = slot(peer_of(z, k, blks), peer_of(x, j, tiles))
            for h in range(2):
                arrived(block, h)
            attend(block)
        repeat(tiles - 1, one)

    repeat(tiles - 1, from_x)
    repeat(blks - 1, from_z)
    repeat(blks - 1, diagonal)

    put_acc[...] = acc[...].astype(jnp.bfloat16)
    lane = lax.broadcasted_iota(jnp.int32, put_stat.shape, 1)
    put_stat[...] = jnp.where(lane < width // 2, stat[0], stat[1])
    send_acc = pltpu.make_async_remote_copy(
        put_acc, got_acc, part_send.at[0], part_recv.at[0],
        device_id={"sub": other}, device_id_type=MESH,
    )
    send_stat = pltpu.make_async_remote_copy(
        put_stat, got_stat, part_send.at[1], part_recv.at[1],
        device_id={"sub": other}, device_id_type=MESH,
    )
    send_stat.start()
    send_acc.start()

    def own_sent(k):
        for r in range(2):
            own_to_z(k, r).wait_send()

    def own_sent_x(k):
        for r in range(2):
            own_to_x(k, r).wait_send()

    def fwd_sent(k):
        def one(j):
            for h in range(2):
                forward(k, j, h).wait_send()
        repeat(tiles - 1, one)

    repeat(blks - 1, own_sent)
    repeat(tiles - 1, own_sent_x)
    repeat(blks - 1, fwd_sent)

    send_stat.wait()
    my_top, my_total = stat[0][:, :1], stat[1][:, :1]
    its_top, its_total = got_stat[:, :1], got_stat[:, width // 2:width // 2 + 1]
    top = jnp.maximum(my_top, its_top)
    mine_by, its_by = jnp.exp(my_top - top), jnp.exp(its_top - top)
    total = my_total * mine_by + its_total * its_by
    mine_by, its_by = mine_by / total, its_by / total
    send_acc.wait()
    gathered = acc[...] * mine_by + got_acc[...].astype(jnp.float32) * its_by
    whole = jnp.concatenate([feats[0], feats[1]], axis=1).astype(jnp.float32)
    mixed = whole + gathered
    squares = jnp.sum(mixed * mixed, axis=1, keepdims=True)
    wanted = jnp.where(s == 0, mixed[:, :width], mixed[:, width:])
    out_ref[...] = wanted * lax.rsqrt(squares + 1e-06)


def local(raw_desc, desc_mean, whitening):
    rows, depth = raw_desc.shape
    width = whitening.shape[1]
    blks, tiles = lax.axis_size("blk"), lax.axis_size("tile")
    chunks = 4
    part = rows // 2
    chips = blks * tiles
    vmem = pl.BlockSpec(memory_space=pltpu.VMEM)
    hbm = pl.BlockSpec(memory_space=pltpu.HBM)
    dma = pltpu.SemaphoreType.DMA
    bf16, f32 = jnp.bfloat16, jnp.float32
    raw_desc = pltpu.with_memory_space_constraint(raw_desc, pltpu.HBM)
    whitening = pltpu.with_memory_space_constraint(whitening, pltpu.HBM)
    return pl.pallas_call(
        functools.partial(kernel, blks, tiles, chunks),
        out_shape=jax.ShapeDtypeStruct((rows, width), f32),
        in_specs=[hbm, vmem, hbm],
        out_specs=vmem,
        scratch_shapes=[
            pltpu.VMEM((rows, depth), bf16),
            pltpu.VMEM((depth, width), bf16),
            pltpu.VMEM((2, rows, width), bf16),
            pltpu.VMEM((chips, 2, part, width), bf16),
            pltpu.VMEM((rows, 2 * width), f32),
            pltpu.VMEM((2, rows, width), f32),
            pltpu.VMEM((rows, 2 * width), bf16),
            pltpu.VMEM((rows, width), f32),
            pltpu.VMEM((rows, 2 * width), bf16),
            pltpu.VMEM((rows, width), f32),
            dma((chunks,)),
            dma,
            dma((2,)),
            dma((2,)),
            dma((blks - 1 + tiles - 1, 2)),
            dma((blks - 1, tiles - 1, 2)),
            dma((chips, 2)),
            dma((2,)),
            dma((2,)),
        ],
        compiler_params=pltpu.CompilerParams(collective_id=0, has_side_effects=True, vmem_limit_bytes=40 * 2 ** 20),
        name="augment",
    )(raw_desc, desc_mean, whitening)


def solution(mesh):
    return jax.shard_map(
        local,
        mesh=mesh,
        in_specs=(P(("groups", "blk", "tile"), None), P(), P(None, "sub")),
        out_specs=P(("groups", "blk", "tile"), "sub"),
        check_vma=False,
    )
```
